32 devices in a mesh: tm: 8 (over y, x, core), chan: 4 (over z).
Axes of the slice: x: 2, y: 2, z: 4, core: 2. Of those that a mesh axis runs over, the one named last changes fastest.
Arguments:
- samples: bfloat16 [2, 16384, 2048], P(None, ('tm', 'chan')), may hold values from -6 to 6
- taps: float32 [8, 2048], replicated, may hold values from -2.5 to 2.5
Outputs:
- spectra: bfloat16 [2, 2, 1024, 16384], P(None, None, ('tm', 'chan'))
The draws below stay inside these ranges and needn't reach their ends.
All inputs are finite; a program needn't handle non-finite values.
Results may differ from the reference program's by a relative error of at most 0.0055.
Values may be sent and summed in bfloat16 or wider, within the bound.
A program may use at most 64 MiB of HBM per device.

```python
import jax
import jax.numpy as jnp
from jax import lax

NFFT = 2048
TAPS = 8
POL = 2
F_DEV = 512
FRAMES = 16384
CHANNELS = 1024


def level_of(key, extent, cuts, low, largest):
    gain, own = 1.0, jax.random.fold_in(key, 6)
    for axis_at, blocks in cuts:
        draws = jnp.exp(jax.random.uniform(jax.random.fold_in(own, axis_at), (blocks,), jnp.float32, low / len(cuts), largest / len(cuts)))
        gain = gain * jnp.repeat(draws, extent[axis_at] // blocks).reshape([-1 if axis == axis_at else 1 for axis in range(len(extent))])
    return gain


def centred(own_key, dims, width, limit, shards=(), kind=jnp.bfloat16):
    entries = jax.random.normal(own_key, dims, jnp.float32) * width
    if len(shards) > 0:
        entries = level_of(own_key, dims, shards, -0.22, 0.18) * entries
    return jnp.clip(entries, min=-limit, max=limit).astype(kind)


def setup_inputs(seed: int = 0) -> dict:
    streams_of = jax.random.split(jax.random.key(seed), 3)
    return {
        "samples": centred(streams_of[0], (POL, FRAMES, NFFT), 1.0, 6.0, ((1, 32),)),
        "taps": centred(streams_of[1], (TAPS, NFFT), 0.35, 2.5, (), jnp.float32),
    }


def make_table(nfft, count):
    index_k = jnp.arange(count, dtype=jnp.int32)[:, None]
    index_n = jnp.arange(nfft, dtype=jnp.int32)[None, :]
    phase = ((index_k * index_n) % nfft).astype(jnp.float32)
    angle = phase * (2.0 * 3.141592653589793 / nfft)
    return jnp.stack([jnp.cos(angle) / 32.0, -jnp.sin(angle) / 32.0]).astype(jnp.bfloat16)


def reference(samples, taps):
    table = make_table(NFFT, CHANNELS).astype(jnp.float32)
    padded = jnp.concatenate([jnp.zeros((POL, TAPS - 1, NFFT), samples.dtype), samples], axis=1)
    blocks = FRAMES // F_DEV

    def one_block(block):
        start = (block * F_DEV).astype(jnp.int32)
        window = lax.dynamic_slice_in_dim(padded, start, F_DEV + TAPS - 1, 1).astype(jnp.float32)
        weighted = jnp.zeros((POL, F_DEV, NFFT), jnp.float32)
        for tap in range(TAPS):
            weighted = weighted + taps[tap][None, None, :] * window[:, tap:tap + F_DEV, :]
        weighted = weighted.astype(jnp.bfloat16).astype(jnp.float32)
        return jnp.einsum('ckn,pfn->cpkf', table, weighted).astype(jnp.bfloat16)

    pieces = lax.map(one_block, jnp.arange(blocks, dtype=jnp.int32))
    pieces = jnp.transpose(pieces, (1, 2, 3, 0, 4))
    return pieces.reshape(2, POL, CHANNELS, FRAMES)
```

```python
import functools

import jax
import jax.numpy as jnp
import numpy as np
from jax import lax
from jax.experimental import pallas as pl
from jax.experimental.pallas import tpu as pltpu
from jax.sharding import PartitionSpec as P

MESH = pl.DeviceIdType.MESH
HALO = 8
ROWS = 128
LANES = 128


def base_tables(nfft, per_dev, count):
    n = np.arange(nfft, dtype=np.int64)[None, :]

    def pair(steps, scale):
        angle = (steps[:, None] * n % nfft) * (2.0 * np.pi / nfft)
        return np.stack([np.cos(angle) * scale, np.sin(angle) * scale]).astype(np.float32)

    coarse = pair(np.arange(count, dtype=np.int64) * per_dev, 1.0 / 32.0)
    fine = pair(np.arange(per_dev, dtype=np.int64), 1.0)
    return coarse, fine


def kernel(
    tms, chans, samples, taps_in, coarse_in, fine_in, out,
    xs, taps, coarse, fine, weighted, table, sp,
    load_sem, base_sem, coarse_sem, halo_sem, own_sem, send_sem, recv_sem,
):
    pols, frames, nfft = samples.shape
    tap_count = taps_in.shape[0]
    per_dev = fine_in.shape[1]
    count = tms * chans
    half = frames // 2
    quarter = frames // 4
    my_tm, my_z = lax.axis_index("tm"), lax.axis_index("chan")
    me = my_tm * chans + my_z

    def group_of(step):
        return lax.bitwise_xor(my_z, lax.bitwise_xor(step, chans // 2))

    def coarse_load(step):
        z = group_of(step)
        return pltpu.make_async_copy(coarse_in.at[z], coarse.at[z], coarse_sem.at[step])

    taps_load = pltpu.make_async_copy(taps_in, taps, base_sem.at[0])
    fine_load = pltpu.make_async_copy(fine_in, fine, base_sem.at[1])
    spans = [
        (0, frames - quarter - HALO, quarter + HALO),
        (0, half - HALO, quarter),
        *((p, half - HALO, half + HALO) for p in range(1, pols)),
        *((p, 0, half - HALO) for p in range(pols)),
    ]
    loads = [
        pltpu.make_async_copy(
            samples.at[p, pl.ds(low, size)], xs.at[p, pl.ds(HALO + low, size)], load_sem.at[at]
        )
        for at, (p, low, size) in enumerate(spans)
    ]
    fine_load.start()
    coarse_load(0).start()
    taps_load.start()
    loads[0].start()

    barrier = pltpu.get_barrier_semaphore()

    for step in range(chans):
        for turn_by in range(tms):
            z, tm = group_of(step), lax.rem(my_tm + turn_by, tms)

            if (step, turn_by) != (chans // 2, 0):
                pl.semaphore_signal(barrier, inc=1, device_id=(tm, z), device_id_type=MESH)

    for step in range(1, chans):
        coarse_load(step).start()
    for load in loads[1:]:
        load.start()

    after = lax.rem(me + 1, count)
    halo = pltpu.make_async_remote_copy(
        src_ref=samples.at[:, pl.ds(frames - HALO, HALO), :],
        dst_ref=xs.at[:, pl.ds(0, HALO), :],
        send_sem=halo_sem.at[0],
        recv_sem=halo_sem.at[1],
        device_id=(after // chans, lax.rem(after, chans)),
        device_id_type=MESH,
    )

    def filter_chunk(p, low, size):
        blocks = size // ROWS
        lane_blocks = nfft // LANES

        def body(step, _):
            row = pl.multiple_of((step // lane_blocks) * ROWS, ROWS)
            lane = pl.multiple_of(lax.rem(step, lane_blocks) * LANES, LANES)
            x = xs[p, pl.ds(low + row, ROWS + HALO), pl.ds(lane, LANES)]
            x = x.astype(jnp.float32)
            w = taps[:, pl.ds(lane, LANES)]
            total = None
            for tap in range(tap_count):
                by = tap_count - 1 - tap
                moved = x if by == 0 else pltpu.roll(x, by, 0)
                term = w[tap : tap + 1, :] * moved[HALO:, :]
                total = term if total is None else total + term
            weighted[pl.ds(row, ROWS), pl.ds(lane, LANES)] = total.astype(jnp.bfloat16)
            return 0

        lax.fori_loop(0, blocks * lane_blocks, body, 0)

    def make_group(z):
        def body(tm, _):
            cos_i, sin_i = coarse[z, 0, pl.ds(tm, 1), :], coarse[z, 1, pl.ds(tm, 1), :]
            cos_j, sin_j = fine[0], fine[1]
            table[z, tm, 0] = (cos_i * cos_j - sin_i * sin_j).astype(jnp.bfloat16)
            table[z, tm, 1] = (-(sin_i * cos_j + cos_i * sin_j)).astype(jnp.bfloat16)
            return 0

        lax.fori_loop(0, tms, body, 0)

    fine_load.wait()
    coarse_load(0).wait()
    make_group(group_of(jnp.int32(0)))

    def chunk(p, low, size, first):
        def group(step, _):
            z = group_of(step)
            rows = table[z].reshape(tms * 2 * per_dev, nfft)
            product = lax.dot_general(
                rows, weighted[pl.ds(0, size), :], (((1,), (1,)), ((), ())),
                preferred_element_type=jnp.float32,
            )
            product = product.reshape(tms, 2, per_dev, size)
            sp[z, :, :, p, :, low : low + size] = product.astype(jnp.bfloat16)
            def send(turn_by, _):
                tm = lax.rem(my_tm + turn_by, tms)
                dest = tm * chans + z

                @pl.when(dest != me)
                def _():
                    pltpu.make_async_remote_copy(
                        src_ref=sp.at[z, tm, :, p, :, pl.ds(low, size)],
                        dst_ref=out.at[:, p, :, pl.ds(pl.multiple_of(me * frames + low, LANES), size)],
                        send_sem=send_sem.at[dest],
                        recv_sem=recv_sem.at[me],
                        device_id=(tm, z),
                        device_id_type=MESH,
                    ).start()

                return 0

            lax.fori_loop(0, tms, send, 0)
            if first:
                @pl.when(step < chans - 1)
                def _():
                    coarse_load(step + 1).wait()
                    make_group(group_of(step + 1))

            return 0

        filter_chunk(p, low, size)
        if first:
            pl.semaphore_wait(barrier, count - 1)
            halo.start()
        lax.fori_loop(0, chans, group, 0)

    taps_load.wait()
    loads[0].wait()
    chunk(0, frames - quarter, quarter, True)
    loads[1].wait()
    chunk(0, half, quarter, False)
    for p in range(1, pols):
        loads[1 + p].wait()
        chunk(p, half, half, False)
    halo.wait()

    @pl.when(me == 0)
    def _():
        xs[:, 0:HALO, :] = jnp.zeros((pols, HALO, nfft), jnp.bfloat16)

    for p in range(pols):
        loads[1 + pols + p].wait()
        chunk(p, 0, half, False)

    own = pltpu.make_async_copy(
        sp.at[my_z, my_tm],
        out.at[:, :, :, pl.ds(pl.multiple_of(me * frames, frames), frames)],
        own_sem,
    )
    own.start()

    def block(z, tm):
        peer = tm * chans + z
        return pltpu.make_async_remote_copy(
            src_ref=sp.at[z, tm],
            dst_ref=out.at[:, :, :, pl.ds(pl.multiple_of(peer * frames, frames), frames)],
            send_sem=send_sem.at[peer],
            recv_sem=recv_sem.at[peer],
            device_id=(tm, z),
            device_id_type=MESH,
        )

    def finish_group(step):
        z = group_of(step)

        def body(turn_by, _):
            block(z, lax.rem(my_tm + turn_by, tms)).wait()
            return 0

        lax.fori_loop(1 if step == chans // 2 else 0, tms, body, 0)

    own.wait()
    for step in reversed(range(chans)):
        finish_group(step)


def local(tms, chans, samples, taps):
    pols, frames, nfft = samples.shape
    tap_count = taps.shape[0]
    count = tms * chans
    per_dev = nfft // 2 // count
    coarse, fine = base_tables(nfft, per_dev, count)
    coarse = coarse.reshape(2, tms, chans, nfft).transpose(2, 0, 1, 3)
    vmem = pl.BlockSpec(memory_space=pltpu.VMEM)
    hbm = pl.BlockSpec(memory_space=pl.ANY)
    return pl.pallas_call(
        functools.partial(kernel, tms, chans),
        out_shape=pltpu.VMEM((2, pols, per_dev, frames * count), jnp.bfloat16),
        in_specs=[hbm, hbm, hbm, hbm],
        out_specs=vmem,
        scratch_shapes=[
            pltpu.VMEM((pols, HALO + frames, nfft), jnp.bfloat16),
            pltpu.VMEM((tap_count, nfft), jnp.float32),
            pltpu.VMEM((chans, 2, tms, nfft), jnp.float32),
            pltpu.VMEM((2, per_dev, nfft), jnp.float32),
            pltpu.VMEM((frames // 2, nfft), jnp.bfloat16),
            pltpu.VMEM((chans, tms, 2, per_dev, nfft), jnp.bfloat16),
            pltpu.VMEM((chans, tms, 2, pols, per_dev, frames), jnp.bfloat16),
            pltpu.SemaphoreType.DMA((2 * pols + 1,)),
            pltpu.SemaphoreType.DMA((2,)),
            pltpu.SemaphoreType.DMA((chans,)),
            pltpu.SemaphoreType.DMA((2,)),
            pltpu.SemaphoreType.DMA,
            pltpu.SemaphoreType.DMA((count,)),
            pltpu.SemaphoreType.DMA((count,)),
        ],
        compiler_params=pltpu.CompilerParams(
            collective_id=0, has_side_effects=True, vmem_limit_bytes=56 * 1024 * 1024
        ),
    )(samples, taps, jnp.asarray(coarse), jnp.asarray(fine))


def solution(mesh):
    return jax.shard_map(
        functools.partial(local, mesh.shape["tm"], mesh.shape["chan"]),
        mesh=mesh,
        in_specs=(P(None, ("tm", "chan"), None), P()),
        out_specs=P(None, None, ("tm", "chan"), None),
        check_vma=False,
    )
```

```python
import functools

import jax
import jax.numpy as jnp
import numpy as np
from jax import lax
from jax.experimental import pallas as pl
from jax.experimental.pallas import tpu as pltpu
from jax.sharding import PartitionSpec as P

MESH = pl.DeviceIdType.MESH
HALO = 8
ROWS = 128
LANES = 128


def base_tables(nfft, per_dev, count):
    n = np.arange(nfft // 2, dtype=np.int64)[None, :]

    def pair(steps, scale):
        angle = (steps[:, None] * n % nfft) * (2.0 * np.pi / nfft)
        return np.stack([np.cos(angle) * scale, np.sin(angle) * scale]).astype(np.float32)

    coarse = pair(np.arange(count, dtype=np.int64) * per_dev, 1.0 / 32.0)
    fine = pair(np.arange(per_dev, dtype=np.int64), 1.0)
    return coarse, fine


def kernel(
    tms, chans, samples, taps_in, coarse_in, fine_in, out,
    xs, taps, coarse, fine, stage, weighted, table, sp,
    load_sem, base_sem, coarse_sem, halo_sem, own_sem, send_sem, recv_sem, met_sem,
):
    pols, frames, nfft = samples.shape
    tap_count = taps_in.shape[0]
    per_dev = fine_in.shape[1]
    count = tms * chans
    half = frames // 2
    quarter = frames // 4
    my_tm, my_z = lax.axis_index("tm"), lax.axis_index("chan")
    me = my_tm * chans + my_z

    def group_of(step):
        return lax.bitwise_xor(my_z, lax.bitwise_xor(step, chans // 2))

    def coarse_load(step):
        z = group_of(step)
        return pltpu.make_async_copy(coarse_in.at[z], coarse.at[z], coarse_sem.at[step])

    taps_load = pltpu.make_async_copy(taps_in, taps, base_sem.at[0])
    fine_load = pltpu.make_async_copy(fine_in, fine, base_sem.at[1])
    spans = [
        (0, frames - quarter - HALO, quarter + HALO),
        (0, half - HALO, quarter),
        *((p, half - HALO, half + HALO) for p in range(1, pols)),
        *((p, 0, half - HALO) for p in range(pols)),
    ]
    loads = [
        pltpu.make_async_copy(
            samples.at[p, pl.ds(low, size)], xs.at[p, pl.ds(HALO + low, size)], load_sem.at[at]
        )
        for at, (p, low, size) in enumerate(spans)
    ]
    fine_load.start()
    coarse_load(0).start()
    taps_load.start()
    loads[0].start()

    barrier = pltpu.get_barrier_semaphore()

    facing, beside = group_of(0), lax.bitwise_xor(my_z, 1)
    before = lax.rem(me + count - 1, count)

    def signal(sem, tm, z):
        pl.semaphore_signal(sem, inc=1, device_id=(tm, z), device_id_type=MESH)

    signal(barrier, before // chans, lax.rem(before, chans))
    signal(barrier, my_tm, beside)
    for turn_by in range(tms):
        signal(barrier, lax.rem(my_tm + turn_by, tms), facing)

    def enter():
        pl.semaphore_wait(barrier, tms + 2)
        signal(met_sem.at[0], my_tm, beside)
        halo.start()

    for step in range(1, chans):
        coarse_load(step).start()
    for load in loads[1:]:
        load.start()

    after = lax.rem(me + 1, count)
    halo = pltpu.make_async_remote_copy(
        src_ref=samples.at[:, pl.ds(frames - HALO, HALO), :],
        dst_ref=xs.at[:, pl.ds(0, HALO), :],
        send_sem=halo_sem.at[0],
        recv_sem=halo_sem.at[1],
        device_id=(after // chans, lax.rem(after, chans)),
        device_id_type=MESH,
    )

    def filter_chunk(p, low, size):
        blocks = size // ROWS
        lane_blocks = nfft // LANES
        slots = stage.shape[0]

        def body(step, _):
            for slot in range(slots):
                at = step * slots + slot
                row = pl.multiple_of((at // lane_blocks) * ROWS, ROWS)
                lane = pl.multiple_of(lax.rem(at, lane_blocks) * LANES, LANES)
                x = xs[p, pl.ds(low + row, ROWS + HALO), pl.ds(lane, LANES)]
                stage[slot] = x.astype(jnp.float32)
                w = taps[:, pl.ds(lane, LANES)]
                total = None
                for tap in range(tap_count):
                    moved = stage[slot, pl.ds(HALO - tap_count + 1 + tap, ROWS), :]
                    term = w[tap : tap + 1, :] * moved
                    total = term if total is None else total + term
                weighted[pl.ds(row, ROWS), pl.ds(lane, LANES)] = total.astype(jnp.bfloat16)
            return 0

        lax.fori_loop(0, blocks * lane_blocks // slots, body, 0)

    def make_group(z):
        def body(tm, _):
            cos_i, sin_i = coarse[z, 0, pl.ds(tm, 1), :], coarse[z, 1, pl.ds(tm, 1), :]
            cos_j, sin_j = fine[0], fine[1]
            channel = (tm * chans + z) * per_dev + lax.broadcasted_iota(jnp.int32, (per_dev, 1), 0)
            sign = (1 - 2 * lax.rem(channel, 2)).astype(jnp.float32)
            for part, values in enumerate(
                (cos_i * cos_j - sin_i * sin_j, -(sin_i * cos_j + cos_i * sin_j))
            ):
                table[z, tm, part, :, 0 : nfft // 2] = values.astype(jnp.bfloat16)
                table[z, tm, part, :, nfft // 2 : nfft] = (values * sign).astype(jnp.bfloat16)
            return 0

        lax.fori_loop(0, tms, body, 0)

    fine_load.wait()
    coarse_load(0).wait()
    make_group(group_of(jnp.int32(0)))

    @pl.when(my_z > chans // 2)
    def _():
        enter()


    def chunk(p, low, size, first):
        def group(step, _):
            z = group_of(step)
            rows = table[z].reshape(tms * 2 * per_dev, nfft)
            product = lax.dot_general(
                rows, weighted[pl.ds(0, size), :], (((1,), (1,)), ((), ())),
                preferred_element_type=jnp.float32,
            )
            product = product.reshape(tms, 2, per_dev, size)
            sp[z, :, :, p, :, low : low + size] = product.astype(jnp.bfloat16)
            if first:
                @pl.when(jnp.logical_and(step == 0, my_z < chans // 2))
                def _():
                    enter()

                @pl.when(step == 1)
                def _():
                    pl.semaphore_wait(met_sem.at[0], 1)
                    signal(met_sem.at[1], my_tm, facing)

                @pl.when(step == chans // 2)
                def _():
                    pl.semaphore_wait(met_sem.at[1], 1)

            def send(turn_by, _):
                tm = lax.rem(my_tm + turn_by, tms)
                dest = tm * chans + z

                @pl.when(dest != me)
                def _():
                    pltpu.make_async_remote_copy(
                        src_ref=sp.at[z, tm, :, p, :, pl.ds(low, size)],
                        dst_ref=out.at[:, p, :, pl.ds(pl.multiple_of(me * frames + low, LANES), size)],
                        send_sem=send_sem.at[dest],
                        recv_sem=recv_sem.at[me],
                        device_id=(tm, z),
                        device_id_type=MESH,
                    ).start()

                return 0

            lax.fori_loop(0, tms, send, 0)
            if first:
                @pl.when(step < chans - 1)
                def _():
                    coarse_load(step + 1).wait()
                    make_group(group_of(step + 1))

            return 0

        filter_chunk(p, low, size)
        if first:
            @pl.when(my_z == chans // 2)
            def _():
                enter()

        lax.fori_loop(0, chans, group, 0)

    taps_load.wait()
    loads[0].wait()
    chunk(0, frames - quarter, quarter, True)
    loads[1].wait()
    chunk(0, half, quarter, False)
    for p in range(1, pols):
        loads[1 + p].wait()
        chunk(p, half, half, False)
    halo.wait()

    @pl.when(me == 0)
    def _():
        xs[:, 0:HALO, :] = jnp.zeros((pols, HALO, nfft), jnp.bfloat16)

    for p in range(pols):
        loads[1 + pols + p].wait()
        chunk(p, 0, half, False)

    own = pltpu.make_async_copy(
        sp.at[my_z, my_tm],
        out.at[:, :, :, pl.ds(pl.multiple_of(me * frames, frames), frames)],
        own_sem,
    )
    own.start()

    def block(z, tm):
        peer = tm * chans + z
        return pltpu.make_async_remote_copy(
            src_ref=sp.at[z, tm],
            dst_ref=out.at[:, :, :, pl.ds(pl.multiple_of(peer * frames, frames), frames)],
            send_sem=send_sem.at[peer],
            recv_sem=recv_sem.at[peer],
            device_id=(tm, z),
            device_id_type=MESH,
        )

    def finish_group(step):
        z = group_of(step)

        def body(turn_by, _):
            block(z, lax.rem(my_tm + turn_by, tms)).wait()
            return 0

        lax.fori_loop(1 if step == chans // 2 else 0, tms, body, 0)

    own.wait()
    for step in reversed(range(chans)):
        finish_group(step)


def local(tms, chans, samples, taps):
    pols, frames, nfft = samples.shape
    tap_count = taps.shape[0]
    count = tms * chans
    per_dev = nfft // 2 // count
    coarse, fine = base_tables(nfft, per_dev, count)
    coarse = coarse.reshape(2, tms, chans, nfft // 2).transpose(2, 0, 1, 3)
    vmem = pl.BlockSpec(memory_space=pltpu.VMEM)
    hbm = pl.BlockSpec(memory_space=pl.ANY)
    return pl.pallas_call(
        functools.partial(kernel, tms, chans),
        out_shape=pltpu.VMEM((2, pols, per_dev, frames * count), jnp.bfloat16),
        in_specs=[hbm, hbm, hbm, hbm],
        out_specs=vmem,
        scratch_shapes=[
            pltpu.VMEM((pols, HALO + frames, nfft), jnp.bfloat16),
            pltpu.VMEM((tap_count, nfft), jnp.float32),
            pltpu.VMEM((chans, 2, tms, nfft // 2), jnp.float32),
            pltpu.VMEM((2, per_dev, nfft // 2), jnp.float32),
            pltpu.VMEM((2, HALO + ROWS, LANES), jnp.float32),
            pltpu.VMEM((frames // 2, nfft), jnp.bfloat16),
            pltpu.VMEM((chans, tms, 2, per_dev, nfft), jnp.bfloat16),
            pltpu.VMEM((chans, tms, 2, pols, per_dev, frames), jnp.bfloat16),
            pltpu.SemaphoreType.DMA((2 * pols + 1,)),
            pltpu.SemaphoreType.DMA((2,)),
            pltpu.SemaphoreType.DMA((chans,)),
            pltpu.SemaphoreType.DMA((2,)),
            pltpu.SemaphoreType.DMA,
            pltpu.SemaphoreType.DMA((count,)),
            pltpu.SemaphoreType.DMA((count,)),
            pltpu.SemaphoreType.REGULAR((2,)),
        ],
        compiler_params=pltpu.CompilerParams(
            collective_id=0, has_side_effects=True, vmem_limit_bytes=56 * 1024 * 1024
        ),
    )(samples, taps, jnp.asarray(coarse), jnp.asarray(fine))


def solution(mesh):
    return jax.shard_map(
        functools.partial(local, mesh.shape["tm"], mesh.shape["chan"]),
        mesh=mesh,
        in_specs=(P(None, ("tm", "chan"), None), P()),
        out_specs=P(None, None, ("tm", "chan"), None),
        check_vma=False,
    )
```

```python
import functools

import jax
import jax.numpy as jnp
import numpy as np
from jax import lax
from jax.experimental import pallas as pl
from jax.experimental.pallas import tpu as pltpu
from jax.sharding import PartitionSpec as P

MESH = pl.DeviceIdType.MESH
HALO = 8
ROWS = 128
LANES = 128


def base_tables(nfft, per_dev, count):
    n = np.arange(nfft // 2, dtype=np.int64)[None, :]

    def pair(steps, scale):
        angle = (steps[:, None] * n % nfft) * (2.0 * np.pi / nfft)
        return np.stack([np.cos(angle) * scale, np.sin(angle) * scale]).astype(np.float32)

    coarse = pair(np.arange(count, dtype=np.int64) * per_dev, 1.0 / 32.0)
    fine = pair(np.arange(per_dev, dtype=np.int64), 1.0)
    return coarse, fine


def kernel(
    tms, chans, samples, taps_in, coarse_in, fine_in, out,
    xs, taps, coarse, fine, stage, weighted, table, sp,
    load_sem, base_sem, coarse_sem, halo_sem, own_sem, send_sem, recv_sem, met_sem,
):
    pols, frames, nfft = samples.shape
    tap_count = taps_in.shape[0]
    per_dev = fine_in.shape[1]
    count = tms * chans
    half = frames // 2
    quarter = frames // 4
    my_tm, my_z = lax.axis_index("tm"), lax.axis_index("chan")
    me = my_tm * chans + my_z

    def group_of(step):
        return lax.bitwise_xor(my_z, lax.bitwise_xor(step, chans // 2))

    near = jnp.where(my_z < chans // 2, chans // 2, chans // 2 - 1)

    def first_group_of(step):
        crossing = step < chans // 2
        return lax.bitwise_xor(jnp.where(crossing, near, my_z), lax.rem(step, chans // 2))

    def coarse_load(step):
        z = first_group_of(step)
        return pltpu.make_async_copy(coarse_in.at[z], coarse.at[z], coarse_sem.at[step])

    taps_load = pltpu.make_async_copy(taps_in, taps, base_sem.at[0])
    fine_load = pltpu.make_async_copy(fine_in, fine, base_sem.at[1])
    spans = [
        (0, frames - quarter - HALO, quarter + HALO),
        (0, half - HALO, quarter),
        *((p, half - HALO, half + HALO) for p in range(1, pols)),
        *((p, 0, half - HALO) for p in range(pols)),
    ]
    loads = [
        pltpu.make_async_copy(
            samples.at[p, pl.ds(low, size)], xs.at[p, pl.ds(HALO + low, size)], load_sem.at[at]
        )
        for at, (p, low, size) in enumerate(spans)
    ]
    fine_load.start()
    coarse_load(0).start()
    taps_load.start()
    loads[0].start()

    barrier = pltpu.get_barrier_semaphore()

    beside = lax.bitwise_xor(my_z, 1)
    inner = jnp.logical_or(my_z == chans // 2 - 1, my_z == chans // 2)
    before = lax.rem(me + count - 1, count)

    def signal(sem, tm, z):
        pl.semaphore_signal(sem, inc=1, device_id=(tm, z), device_id_type=MESH)

    signal(barrier, before // chans, lax.rem(before, chans))
    signal(barrier, my_tm, beside)

    @pl.when(inner)
    def _():
        for other in range(chans // 2):
            for turn_by in range(tms):
                signal(barrier, lax.rem(my_tm + turn_by, tms), lax.bitwise_xor(near, other))

    def enter():
        pl.semaphore_wait(barrier, tms + 2)
        halo.start()

        @pl.when(inner)
        def _():
            for turn_by in range(tms):
                signal(met_sem.at[0], lax.rem(my_tm + turn_by, tms), near)

    def meet(at, waits):
        @pl.when(inner)
        def _():
            pl.semaphore_wait(met_sem.at[at], waits)
            signal(met_sem.at[at], my_tm, beside)

        @pl.when(jnp.logical_not(inner))
        def _():
            pl.semaphore_wait(met_sem.at[at], 1)

    after = lax.rem(me + 1, count)
    halo = pltpu.make_async_remote_copy(
        src_ref=samples.at[:, pl.ds(frames - HALO, HALO), :],
        dst_ref=xs.at[:, pl.ds(0, HALO), :],
        send_sem=halo_sem.at[0],
        recv_sem=halo_sem.at[1],
        device_id=(after // chans, lax.rem(after, chans)),
        device_id_type=MESH,
    )

    def filter_chunk(p, low, size):
        blocks = size // ROWS
        lane_blocks = nfft // LANES
        slots = stage.shape[0]

        def body(step, _):
            for slot in range(slots):
                at = step * slots + slot
                row = pl.multiple_of((at // lane_blocks) * ROWS, ROWS)
                lane = pl.multiple_of(lax.rem(at, lane_blocks) * LANES, LANES)
                x = xs[p, pl.ds(low + row, ROWS + HALO), pl.ds(lane, LANES)]
                stage[slot] = x.astype(jnp.float32)
                w = taps[:, pl.ds(lane, LANES)]
                total = None
                for tap in range(tap_count):
                    moved = stage[slot, pl.ds(HALO - tap_count + 1 + tap, ROWS), :]
                    term = w[tap : tap + 1, :] * moved
                    total = term if total is None else total + term
                weighted[pl.ds(row, ROWS), pl.ds(lane, LANES)] = total.astype(jnp.bfloat16)
            return 0

        lax.fori_loop(0, blocks * lane_blocks // slots, body, 0)

    base = my_tm

    def turned(turn_by):
        return lax.rem(base + turn_by, tms)

    def make_tables(z, start, width):
        def body(turn_by, _):
            tm = turned(turn_by)
            cos_i, sin_i = coarse[z, 0, pl.ds(tm, 1), :], coarse[z, 1, pl.ds(tm, 1), :]
            cos_j, sin_j = fine[0], fine[1]
            channel = (tm * chans + z) * per_dev + lax.broadcasted_iota(jnp.int32, (per_dev, 1), 0)
            sign = (1 - 2 * lax.rem(channel, 2)).astype(jnp.float32)
            for part, values in enumerate(
                (cos_i * cos_j - sin_i * sin_j, -(sin_i * cos_j + cos_i * sin_j))
            ):
                table[z, turn_by, part, :, 0 : nfft // 2] = values.astype(jnp.bfloat16)
                table[z, turn_by, part, :, nfft // 2 : nfft] = (values * sign).astype(jnp.bfloat16)
            return 0

        lax.fori_loop(start, start + width, body, 0)

    def transform(p, low, size, z, start, width):
        rows = table[z, start : start + width].reshape(width * 2 * per_dev, nfft)
        product = lax.dot_general(
            rows, weighted[pl.ds(0, size), :], (((1,), (1,)), ((), ())),
            preferred_element_type=jnp.float32,
        )
        product = product.reshape(width, 2, per_dev, size)
        sp[z, start : start + width, :, p, :, low : low + size] = product.astype(jnp.bfloat16)

    def send(p, low, size, z, start, width):
        def body(turn_by, _):
            tm = turned(turn_by)
            dest = tm * chans + z

            @pl.when(dest != me)
            def _():
                pltpu.make_async_remote_copy(
                    src_ref=sp.at[z, turn_by, :, p, :, pl.ds(low, size)],
                    dst_ref=out.at[:, p, :, pl.ds(pl.multiple_of(me * frames + low, LANES), size)],
                    send_sem=send_sem.at[dest],
                    recv_sem=recv_sem.at[me],
                    device_id=(tm, z),
                    device_id_type=MESH,
                ).start()

            return 0

        lax.fori_loop(start, start + width, body, 0)

    def first_chunk(p, low, size):
        fine_load.wait()
        coarse_load(0).wait()
        for step in range(1, chans):
            coarse_load(step).start()
        for load in loads[1:]:
            load.start()
        make_tables(near, 0, lead)

        @pl.when(my_z > chans // 2)
        def _():
            enter()

        taps_load.wait()
        loads[0].wait()
        filter_chunk(p, low, size)

        @pl.when(inner)
        def _():
            enter()

        transform(p, low, size, near, 0, lead)

        @pl.when(my_z < chans // 2 - 1)
        def _():
            enter()

        send(p, low, size, near, 0, lead)
        if lead < tms:
            make_tables(near, lead, tms - lead)
            transform(p, low, size, near, lead, tms - lead)
            send(p, low, size, near, lead, tms - lead)

        def group(step, _):
            z = first_group_of(step)
            coarse_load(step).wait()
            make_tables(z, 0, tms)
            transform(p, low, size, z, 0, tms)

            @pl.when(step == 1)
            def _():
                meet(0, tms)

                @pl.when(inner)
                def _():
                    for turn_by in range(1, tms):
                        signal(met_sem.at[1], lax.rem(my_tm + turn_by, tms), my_z)

            @pl.when(step == chans // 2)
            def _():
                meet(1, tms - 1)

            send(p, low, size, z, 0, tms)
            return 0

        lax.fori_loop(1, chans, group, 0)

    def chunk(p, low, size):
        def group(step, _):
            z = group_of(step)
            transform(p, low, size, z, 0, tms)
            send(p, low, size, z, 0, tms)
            return 0

        filter_chunk(p, low, size)
        lax.fori_loop(0, chans, group, 0)

    lead = max(tms // 4, 1)
    first_chunk(0, frames - quarter, quarter)
    loads[1].wait()
    chunk(0, half, quarter)
    for p in range(1, pols):
        loads[1 + p].wait()
        chunk(p, half, half)
    halo.wait()

    @pl.when(me == 0)
    def _():
        xs[:, 0:HALO, :] = jnp.zeros((pols, HALO, nfft), jnp.bfloat16)

    for p in range(pols):
        loads[1 + pols + p].wait()
        chunk(p, 0, half)

    own = pltpu.make_async_copy(
        sp.at[my_z, 0],
        out.at[:, :, :, pl.ds(pl.multiple_of(me * frames, frames), frames)],
        own_sem,
    )
    own.start()

    def finish_group(step):
        z = group_of(step)

        def body(turn_by, _):
            tm = turned(turn_by)
            peer = tm * chans + z

            @pl.when(peer != me)
            def _():
                pltpu.make_async_remote_copy(
                    src_ref=sp.at[z, turn_by],
                    dst_ref=out.at[:, :, :, pl.ds(pl.multiple_of(peer * frames, frames), frames)],
                    send_sem=send_sem.at[peer],
                    recv_sem=recv_sem.at[peer],
                    device_id=(tm, z),
                    device_id_type=MESH,
                ).wait()

            return 0

        lax.fori_loop(0, tms, body, 0)

    own.wait()
    for step in reversed(range(chans)):
        finish_group(step)


def local(tms, chans, samples, taps):
    pols, frames, nfft = samples.shape
    tap_count = taps.shape[0]
    count = tms * chans
    per_dev = nfft // 2 // count
    coarse, fine = base_tables(nfft, per_dev, count)
    coarse = coarse.reshape(2, tms, chans, nfft // 2).transpose(2, 0, 1, 3)
    vmem = pl.BlockSpec(memory_space=pltpu.VMEM)
    hbm = pl.BlockSpec(memory_space=pl.ANY)
    return pl.pallas_call(
        functools.partial(kernel, tms, chans),
        out_shape=pltpu.VMEM((2, pols, per_dev, frames * count), jnp.bfloat16),
        in_specs=[hbm, hbm, hbm, hbm],
        out_specs=vmem,
        scratch_shapes=[
            pltpu.VMEM((pols, HALO + frames, nfft), jnp.bfloat16),
            pltpu.VMEM((tap_count, nfft), jnp.float32),
            pltpu.VMEM((chans, 2, tms, nfft // 2), jnp.float32),
            pltpu.VMEM((2, per_dev, nfft // 2), jnp.float32),
            pltpu.VMEM((2, HALO + ROWS, LANES), jnp.float32),
            pltpu.VMEM((frames // 2, nfft), jnp.bfloat16),
            pltpu.VMEM((chans, tms, 2, per_dev, nfft), jnp.bfloat16),
            pltpu.VMEM((chans, tms, 2, pols, per_dev, frames), jnp.bfloat16),
            pltpu.SemaphoreType.DMA((2 * pols + 1,)),
            pltpu.SemaphoreType.DMA((2,)),
            pltpu.SemaphoreType.DMA((chans,)),
            pltpu.SemaphoreType.DMA((2,)),
            pltpu.SemaphoreType.DMA,
            pltpu.SemaphoreType.DMA((count,)),
            pltpu.SemaphoreType.DMA((count,)),
            pltpu.SemaphoreType.REGULAR((2,)),
        ],
        compiler_params=pltpu.CompilerParams(
            collective_id=0, has_side_effects=True, vmem_limit_bytes=56 * 1024 * 1024
        ),
    )(samples, taps, jnp.asarray(coarse), jnp.asarray(fine))


def solution(mesh):
    return jax.shard_map(
        functools.partial(local, mesh.shape["tm"], mesh.shape["chan"]),
        mesh=mesh,
        in_specs=(P(None, ("tm", "chan"), None), P()),
        out_specs=P(None, None, ("tm", "chan"), None),
        check_vma=False,
    )
```

```python
import functools

import jax
import jax.numpy as jnp
import numpy as np
from jax import lax
from jax.experimental import pallas as pl
from jax.experimental.pallas import tpu as pltpu
from jax.sharding import PartitionSpec as P

MESH = pl.DeviceIdType.MESH
HALO = 8
ROWS = 128
LANES = 128


def base_tables(nfft, per_dev, count):
    n = np.arange(nfft // 2, dtype=np.int64)[None, :]

    def pair(steps, scale):
        angle = (steps[:, None] * n % nfft) * (2.0 * np.pi / nfft)
        return np.stack([np.cos(angle) * scale, np.sin(angle) * scale]).astype(np.float32)

    coarse = pair(np.arange(count, dtype=np.int64) * per_dev, 1.0 / 32.0)
    fine = pair(np.arange(per_dev, dtype=np.int64), 1.0)
    return coarse, fine


def kernel(
    tms, chans, samples, taps_in, coarse_in, fine_in, out,
    xs, taps, coarse, fine, stage, weighted, table, sp,
    load_sem, base_sem, coarse_sem, halo_sem, own_sem, send_sem, recv_sem, met_sem,
):
    pols, frames, nfft = samples.shape
    tap_count = taps_in.shape[0]
    per_dev = fine_in.shape[1]
    count = tms * chans
    half = frames // 2
    quarter = frames // 4
    my_tm, my_z = lax.axis_index("tm"), lax.axis_index("chan")
    me = my_tm * chans + my_z

    def group_of(step):
        return lax.bitwise_xor(my_z, lax.bitwise_xor(step, chans // 2))

    near = jnp.where(my_z < chans // 2, chans // 2, chans // 2 - 1)

    def first_group_of(step):
        crossing = step < chans // 2
        return lax.bitwise_xor(jnp.where(crossing, near, my_z), lax.rem(step, chans // 2))

    def coarse_load(step):
        z = first_group_of(step)
        return pltpu.make_async_copy(coarse_in.at[z], coarse.at[z], coarse_sem.at[step])

    taps_load = pltpu.make_async_copy(taps_in, taps, base_sem.at[0])
    fine_load = pltpu.make_async_copy(fine_in, fine, base_sem.at[1])
    spans = [
        (0, frames - quarter - HALO, quarter + HALO),
        (0, half - HALO, quarter),
        *((p, half - HALO, half) for p in range(1, pols)),
        *((p, 0, half - HALO) for p in range(pols)),
    ]
    loads = [
        pltpu.make_async_copy(
            samples.at[p, pl.ds(low, size)], xs.at[p, pl.ds(HALO + low, size)], load_sem.at[at]
        )
        for at, (p, low, size) in enumerate(spans)
    ]
    tail_load = pltpu.make_async_copy(
        samples.at[1:pols, pl.ds(frames - HALO, HALO)],
        xs.at[1:pols, pl.ds(frames, HALO)],
        base_sem.at[2],
    )
    fine_load.start()
    coarse_load(0).start()
    taps_load.start()
    loads[0].start()
    tail_load.start()

    barrier = pltpu.get_barrier_semaphore()

    beside = lax.bitwise_xor(my_z, 1)
    inner = jnp.logical_or(my_z == chans // 2 - 1, my_z == chans // 2)
    before = lax.rem(me + count - 1, count)

    def signal(sem, tm, z):
        pl.semaphore_signal(sem, inc=1, device_id=(tm, z), device_id_type=MESH)

    signal(barrier, before // chans, lax.rem(before, chans))
    signal(barrier, my_tm, beside)

    @pl.when(inner)
    def _():
        for other in range(chans // 2):
            for turn_by in range(tms):
                signal(barrier, lax.rem(my_tm + turn_by, tms), lax.bitwise_xor(near, other))

    def enter():
        pl.semaphore_wait(barrier, tms + 2)
        halo.start()

        @pl.when(inner)
        def _():
            for turn_by in range(tms):
                signal(met_sem.at[0], lax.rem(my_tm + turn_by, tms), near)

    def meet(at, waits):
        @pl.when(inner)
        def _():
            pl.semaphore_wait(met_sem.at[at], waits)
            signal(met_sem.at[at], my_tm, beside)

        @pl.when(jnp.logical_not(inner))
        def _():
            pl.semaphore_wait(met_sem.at[at], 1)

    after = lax.rem(me + 1, count)
    halo = pltpu.make_async_remote_copy(
        src_ref=xs.at[:, pl.ds(frames, HALO), :],
        dst_ref=xs.at[:, pl.ds(0, HALO), :],
        send_sem=halo_sem.at[0],
        recv_sem=halo_sem.at[1],
        device_id=(after // chans, lax.rem(after, chans)),
        device_id_type=MESH,
    )

    def filter_chunk(p, low, size):
        blocks = size // ROWS
        lane_blocks = nfft // LANES
        slots = stage.shape[0]

        def body(step, _):
            for slot in range(slots):
                at = step * slots + slot
                row = pl.multiple_of((at // lane_blocks) * ROWS, ROWS)
                lane = pl.multiple_of(lax.rem(at, lane_blocks) * LANES, LANES)
                x = xs[p, pl.ds(low + row, ROWS + HALO), pl.ds(lane, LANES)]
                stage[slot] = x.astype(jnp.float32)
                w = taps[:, pl.ds(lane, LANES)]
                total = None
                for tap in range(tap_count):
                    moved = stage[slot, pl.ds(HALO - tap_count + 1 + tap, ROWS), :]
                    term = w[tap : tap + 1, :] * moved
                    total = term if total is None else total + term
                weighted[pl.ds(row, ROWS), pl.ds(lane, LANES)] = total.astype(jnp.bfloat16)
            return 0

        lax.fori_loop(0, blocks * lane_blocks // slots, body, 0)

    base = my_tm

    def turned(turn_by):
        return lax.rem(base + turn_by, tms)

    def make_tables(z, start, width):
        def body(turn_by, _):
            tm = turned(turn_by)
            cos_i, sin_i = coarse[z, 0, pl.ds(tm, 1), :], coarse[z, 1, pl.ds(tm, 1), :]
            cos_j, sin_j = fine[0], fine[1]
            channel = (tm * chans + z) * per_dev + lax.broadcasted_iota(jnp.int32, (per_dev, 1), 0)
            sign = (1 - 2 * lax.rem(channel, 2)).astype(jnp.float32)
            for part, values in enumerate(
                (cos_i * cos_j - sin_i * sin_j, -(sin_i * cos_j + cos_i * sin_j))
            ):
                table[z, turn_by, part, :, 0 : nfft // 2] = values.astype(jnp.bfloat16)
                table[z, turn_by, part, :, nfft // 2 : nfft] = (values * sign).astype(jnp.bfloat16)
            return 0

        lax.fori_loop(start, start + width, body, 0)

    def transform(p, low, size, z, start, width):
        rows = table[z, start : start + width].reshape(width * 2 * per_dev, nfft)
        product = lax.dot_general(
            rows, weighted[pl.ds(0, size), :], (((1,), (1,)), ((), ())),
            preferred_element_type=jnp.float32,
        )
        product = product.reshape(width, 2, per_dev, size)
        sp[z, start : start + width, :, p, :, low : low + size] = product.astype(jnp.bfloat16)

    def send(p, low, size, z, start, width, halves=False):
        def body(step, _):
            turn_by = step
            if halves:
                part = tms // 2
                tm = step // part * part + lax.rem(my_tm + step, part)
                turn_by = lax.rem(tm - my_tm + tms, tms)

            tm = turned(turn_by)
            dest = tm * chans + z

            @pl.when(dest != me)
            def _():
                pltpu.make_async_remote_copy(
                    src_ref=sp.at[z, turn_by, :, p, :, pl.ds(low, size)],
                    dst_ref=out.at[:, p, :, pl.ds(pl.multiple_of(me * frames + low, LANES), size)],
                    send_sem=send_sem.at[dest],
                    recv_sem=recv_sem.at[me],
                    device_id=(tm, z),
                    device_id_type=MESH,
                ).start()

            return 0

        lax.fori_loop(start, start + width, body, 0)

    def first_chunk(p, low, size):
        fine_load.wait()
        coarse_load(0).wait()
        for step in range(1, chans):
            coarse_load(step).start()
        for load in loads[1:]:
            load.start()
        taps_load.wait()
        tail_load.wait()
        loads[0].wait()

        @pl.when(my_z > chans // 2)
        def _():
            enter()

        make_tables(near, 0, lead)
        filter_chunk(p, low, size)

        @pl.when(inner)
        def _():
            enter()

        transform(p, low, size, near, 0, lead)

        @pl.when(my_z < chans // 2 - 1)
        def _():
            enter()

        send(p, low, size, near, 0, lead)
        if lead < tms:
            make_tables(near, lead, tms - lead)
            transform(p, low, size, near, lead, tms - lead)
            send(p, low, size, near, lead, tms - lead)

        def group(step, _):
            z = first_group_of(step)
            coarse_load(step).wait()
            make_tables(z, 0, tms)
            transform(p, low, size, z, 0, tms)

            @pl.when(step == 1)
            def _():
                meet(0, tms)

                @pl.when(inner)
                def _():
                    for turn_by in range(1, tms):
                        signal(met_sem.at[1], lax.rem(my_tm + turn_by, tms), my_z)

            @pl.when(step == chans // 2)
            def _():
                meet(1, tms - 1)

            send(p, low, size, z, 0, tms)
            return 0

        lax.fori_loop(1, chans, group, 0)

    def chunk(p, low, size):
        def group(step, _):
            z = group_of(step)
            transform(p, low, size, z, 0, tms)
            send(p, low, size, z, 0, tms, p == pols - 1 and low == 0)
            return 0

        filter_chunk(p, low, size)
        lax.fori_loop(0, chans, group, 0)

    lead = max(tms // 4, 1)
    first_chunk(0, frames - quarter, quarter)
    loads[1].wait()
    chunk(0, half, quarter)
    for p in range(1, pols):
        loads[1 + p].wait()
        chunk(p, half, half)
    halo.wait()

    @pl.when(me == 0)
    def _():
        xs[:, 0:HALO, :] = jnp.zeros((pols, HALO, nfft), jnp.bfloat16)

    for p in range(pols):
        loads[1 + pols + p].wait()
        chunk(p, 0, half)

    own = pltpu.make_async_copy(
        sp.at[my_z, 0],
        out.at[:, :, :, pl.ds(pl.multiple_of(me * frames, frames), frames)],
        own_sem,
    )
    own.start()

    def finish_group(step):
        z = group_of(step)

        def body(turn_by, _):
            tm = turned(turn_by)
            peer = tm * chans + z

            @pl.when(peer != me)
            def _():
                pltpu.make_async_remote_copy(
                    src_ref=sp.at[z, turn_by],
                    dst_ref=out.at[:, :, :, pl.ds(pl.multiple_of(peer * frames, frames), frames)],
                    send_sem=send_sem.at[peer],
                    recv_sem=recv_sem.at[peer],
                    device_id=(tm, z),
                    device_id_type=MESH,
                ).wait()

            return 0

        lax.fori_loop(0, tms, body, 0)

    own.wait()
    for step in [*range(2, chans), 0, 1]:
        finish_group(step)


def local(tms, chans, samples, taps):
    pols, frames, nfft = samples.shape
    tap_count = taps.shape[0]
    count = tms * chans
    per_dev = nfft // 2 // count
    coarse, fine = base_tables(nfft, per_dev, count)
    coarse = coarse.reshape(2, tms, chans, nfft // 2).transpose(2, 0, 1, 3)
    vmem = pl.BlockSpec(memory_space=pltpu.VMEM)
    hbm = pl.BlockSpec(memory_space=pl.ANY)
    return pl.pallas_call(
        functools.partial(kernel, tms, chans),
        out_shape=pltpu.VMEM((2, pols, per_dev, frames * count), jnp.bfloat16),
        in_specs=[hbm, hbm, hbm, hbm],
        out_specs=vmem,
        scratch_shapes=[
            pltpu.VMEM((pols, HALO + frames, nfft), jnp.bfloat16),
            pltpu.VMEM((tap_count, nfft), jnp.float32),
            pltpu.VMEM((chans, 2, tms, nfft // 2), jnp.float32),
            pltpu.VMEM((2, per_dev, nfft // 2), jnp.float32),
            pltpu.VMEM((2, HALO + ROWS, LANES), jnp.float32),
            pltpu.VMEM((frames // 2, nfft), jnp.bfloat16),
            pltpu.VMEM((chans, tms, 2, per_dev, nfft), jnp.bfloat16),
            pltpu.VMEM((chans, tms, 2, pols, per_dev, frames), jnp.bfloat16),
            pltpu.SemaphoreType.DMA((2 * pols + 1,)),
            pltpu.SemaphoreType.DMA((3,)),
            pltpu.SemaphoreType.DMA((chans,)),
            pltpu.SemaphoreType.DMA((2,)),
            pltpu.SemaphoreType.DMA,
            pltpu.SemaphoreType.DMA((count,)),
            pltpu.SemaphoreType.DMA((count,)),
            pltpu.SemaphoreType.REGULAR((2,)),
        ],
        compiler_params=pltpu.CompilerParams(
            collective_id=0, has_side_effects=True, vmem_limit_bytes=56 * 1024 * 1024
        ),
    )(samples, taps, jnp.asarray(coarse), jnp.asarray(fine))


def solution(mesh):
    return jax.shard_map(
        functools.partial(local, mesh.shape["tm"], mesh.shape["chan"]),
        mesh=mesh,
        in_specs=(P(None, ("tm", "chan"), None), P()),
        out_specs=P(None, None, ("tm", "chan"), None),
        check_vma=False,
    )
```

```python
import functools

import jax
import jax.numpy as jnp
import numpy as np
from jax import lax
from jax.experimental import pallas as pl
from jax.experimental.pallas import tpu as pltpu
from jax.sharding import PartitionSpec as P

MESH = pl.DeviceIdType.MESH
HALO = 8
ROWS = 128
LANES = 128


def base_tables(nfft, per_dev, count):
    n = np.arange(nfft // 2, dtype=np.int64)[None, :]

    def pair(steps, scale):
        angle = (steps[:, None] * n % nfft) * (2.0 * np.pi / nfft)
        return np.stack([np.cos(angle) * scale, np.sin(angle) * scale]).astype(np.float32)

    coarse = pair(np.arange(count, dtype=np.int64) * per_dev, 1.0 / 32.0)
    fine = pair(np.arange(per_dev, dtype=np.int64), 1.0)
    return coarse, fine


def kernel(
    tms, chans, samples, taps_in, coarse_in, fine_in, out,
    xs, taps, coarse, fine, stage, weighted, table, sp,
    load_sem, base_sem, coarse_sem, halo_sem, own_sem, send_sem, recv_sem, met_sem,
):
    pols, frames, nfft = samples.shape
    tap_count = taps_in.shape[0]
    per_dev = fine_in.shape[1]
    count = tms * chans
    half = frames // 2
    quarter = frames // 4
    my_tm, my_z = lax.axis_index("tm"), lax.axis_index("chan")
    me = my_tm * chans + my_z

    def group_of(step):
        return lax.bitwise_xor(my_z, lax.bitwise_xor(step, chans // 2))

    near = jnp.where(my_z < chans // 2, chans // 2, chans // 2 - 1)

    def first_group_of(step):
        crossing = step < chans // 2
        return lax.bitwise_xor(jnp.where(crossing, near, my_z), lax.rem(step, chans // 2))

    def coarse_load(step):
        z = first_group_of(step)
        return pltpu.make_async_copy(coarse_in.at[z], coarse.at[z], coarse_sem.at[step])

    taps_load = pltpu.make_async_copy(taps_in, taps, base_sem.at[0])
    fine_load = pltpu.make_async_copy(fine_in, fine, base_sem.at[1])
    spans = [
        (0, frames - quarter - HALO, quarter + HALO),
        (0, half - HALO, quarter),
        *((p, half - HALO, half) for p in range(1, pols)),
        *((p, 0, half - HALO) for p in range(pols)),
    ]
    loads = [
        pltpu.make_async_copy(
            samples.at[p, pl.ds(low, size)], xs.at[p, pl.ds(HALO + low, size)], load_sem.at[at]
        )
        for at, (p, low, size) in enumerate(spans)
    ]
    tail_load = pltpu.make_async_copy(
        samples.at[1:pols, pl.ds(frames - HALO, HALO)],
        xs.at[1:pols, pl.ds(frames, HALO)],
        base_sem.at[2],
    )
    fine_load.start()
    coarse_load(0).start()
    taps_load.start()
    loads[0].start()
    tail_load.start()

    barrier = pltpu.get_barrier_semaphore()

    beside = lax.bitwise_xor(my_z, 1)
    inner = jnp.logical_or(my_z == chans // 2 - 1, my_z == chans // 2)
    before = lax.rem(me + count - 1, count)

    def signal(sem, tm, z):
        pl.semaphore_signal(sem, inc=1, device_id=(tm, z), device_id_type=MESH)

    signal(barrier, before // chans, lax.rem(before, chans))
    signal(barrier, my_tm, beside)

    @pl.when(inner)
    def _():
        for other in range(chans // 2):
            for turn_by in range(tms):
                signal(barrier, lax.rem(my_tm + turn_by, tms), lax.bitwise_xor(near, other))

    def enter():
        pl.semaphore_wait(barrier, tms + 2)
        halo.start()

        @pl.when(inner)
        def _():
            for turn_by in range(tms):
                signal(met_sem.at[0], lax.rem(my_tm + turn_by, tms), near)

    def meet(at, waits):
        @pl.when(inner)
        def _():
            pl.semaphore_wait(met_sem.at[at], waits)
            signal(met_sem.at[at], my_tm, beside)

        @pl.when(jnp.logical_not(inner))
        def _():
            pl.semaphore_wait(met_sem.at[at], 1)

    after = lax.rem(me + 1, count)
    halo = pltpu.make_async_remote_copy(
        src_ref=xs.at[:, pl.ds(frames, HALO), :],
        dst_ref=xs.at[:, pl.ds(0, HALO), :],
        send_sem=halo_sem.at[0],
        recv_sem=halo_sem.at[1],
        device_id=(after // chans, lax.rem(after, chans)),
        device_id_type=MESH,
    )

    def filter_chunk(p, low, size):
        blocks = size // ROWS
        lane_blocks = nfft // LANES
        slots = stage.shape[0]

        def body(step, _):
            for slot in range(slots):
                at = step * slots + slot
                row = pl.multiple_of((at // lane_blocks) * ROWS, ROWS)
                lane = pl.multiple_of(lax.rem(at, lane_blocks) * LANES, LANES)
                x = xs[p, pl.ds(low + row, ROWS + HALO), pl.ds(lane, LANES)]
                stage[slot] = x.astype(jnp.float32)
                w = taps[:, pl.ds(lane, LANES)]
                total = None
                for tap in range(tap_count):
                    moved = stage[slot, pl.ds(HALO - tap_count + 1 + tap, ROWS), :]
                    term = w[tap : tap + 1, :] * moved
                    total = term if total is None else total + term
                weighted[pl.ds(row, ROWS), pl.ds(lane, LANES)] = total.astype(jnp.bfloat16)
            return 0

        lax.fori_loop(0, blocks * lane_blocks // slots, body, 0)

    base = my_tm

    def turned(turn_by):
        return lax.rem(base + turn_by, tms)

    def make_tables(z, start, width):
        def body(turn_by, _):
            tm = turned(turn_by)
            cos_i, sin_i = coarse[z, 0, pl.ds(tm, 1), :], coarse[z, 1, pl.ds(tm, 1), :]
            cos_j, sin_j = fine[0], fine[1]
            channel = (tm * chans + z) * per_dev + lax.broadcasted_iota(jnp.int32, (per_dev, 1), 0)
            sign = (1 - 2 * lax.rem(channel, 2)).astype(jnp.float32)
            for part, values in enumerate(
                (cos_i * cos_j - sin_i * sin_j, -(sin_i * cos_j + cos_i * sin_j))
            ):
                table[z, turn_by, part, :, 0 : nfft // 2] = values.astype(jnp.bfloat16)
                table[z, turn_by, part, :, nfft // 2 : nfft] = (values * sign).astype(jnp.bfloat16)
            return 0

        lax.fori_loop(start, start + width, body, 0)

    def transform(p, low, size, z, start, width):
        rows = table[z, start : start + width].reshape(width * 2 * per_dev, nfft)
        product = lax.dot_general(
            rows, weighted[pl.ds(0, size), :], (((1,), (1,)), ((), ())),
            preferred_element_type=jnp.float32,
        )
        product = product.reshape(width, 2, per_dev, size)
        sp[z, start : start + width, :, p, :, low : low + size] = product.astype(jnp.bfloat16)

    def send(p, low, size, z, start, width, halves=False):
        def body(step, _):
            turn_by = step
            if halves:
                part = tms // 2
                tm = step // part * part + lax.rem(my_tm + step, part)
                turn_by = lax.rem(tm - my_tm + tms, tms)

            tm = turned(turn_by)
            dest = tm * chans + z

            @pl.when(dest != me)
            def _():
                pltpu.make_async_remote_copy(
                    src_ref=sp.at[z, turn_by, :, p, :, pl.ds(low, size)],
                    dst_ref=out.at[:, p, :, pl.ds(pl.multiple_of(me * frames + low, LANES), size)],
                    send_sem=send_sem.at[dest],
                    recv_sem=recv_sem.at[me],
                    device_id=(tm, z),
                    device_id_type=MESH,
                ).start()

            return 0

        lax.fori_loop(start, start + width, body, 0)

    def first_chunk(p, low, size):
        fine_load.wait()
        coarse_load(0).wait()
        for step in range(1, chans):
            coarse_load(step).start()
        for load in loads[1:]:
            load.start()
        taps_load.wait()
        tail_load.wait()
        loads[0].wait()

        @pl.when(my_z > chans // 2)
        def _():
            enter()

        make_tables(near, 0, lead)
        filter_chunk(p, low, size)

        @pl.when(inner)
        def _():
            enter()

        transform(p, low, size, near, 0, lead)

        @pl.when(my_z < chans // 2 - 1)
        def _():
            enter()

        send(p, low, size, near, 0, lead)
        if lead < tms:
            make_tables(near, lead, tms - lead)
            transform(p, low, size, near, lead, tms - lead)
            send(p, low, size, near, lead, tms - lead)

        def group(step, _):
            z = first_group_of(step)
            coarse_load(step).wait()
            make_tables(z, 0, tms)
            transform(p, low, size, z, 0, tms)

            @pl.when(step == 1)
            def _():
                meet(0, tms)

                @pl.when(inner)
                def _():
                    for turn_by in range(1, tms):
                        signal(met_sem.at[1], lax.rem(my_tm + turn_by, tms), my_z)

            @pl.when(step == chans // 2)
            def _():
                meet(1, tms - 1)

            send(p, low, size, z, 0, tms)
            return 0

        lax.fori_loop(1, chans, group, 0)

    def chunk(p, low, size):
        def group(step, _):
            z = group_of(step)
            transform(p, low, size, z, 0, tms)
            send(p, low, size, z, 0, tms, True)
            return 0

        filter_chunk(p, low, size)
        lax.fori_loop(0, chans, group, 0)

    lead = max(tms // 4, 1)
    first_chunk(0, frames - quarter, quarter)
    loads[1].wait()
    chunk(0, half, quarter)
    for p in range(1, pols):
        loads[1 + p].wait()
        chunk(p, half, half)
    halo.wait()

    @pl.when(me == 0)
    def _():
        xs[:, 0:HALO, :] = jnp.zeros((pols, HALO, nfft), jnp.bfloat16)

    for p in range(pols):
        loads[1 + pols + p].wait()
        chunk(p, 0, half)

    own = pltpu.make_async_copy(
        sp.at[my_z, 0],
        out.at[:, :, :, pl.ds(pl.multiple_of(me * frames, frames), frames)],
        own_sem,
    )
    own.start()

    def finish_group(step):
        z = group_of(step)

        def body(turn_by, _):
            tm = turned(turn_by)
            peer = tm * chans + z

            @pl.when(peer != me)
            def _():
                pltpu.make_async_remote_copy(
                    src_ref=sp.at[z, turn_by],
                    dst_ref=out.at[:, :, :, pl.ds(pl.multiple_of(peer * frames, frames), frames)],
                    send_sem=send_sem.at[peer],
                    recv_sem=recv_sem.at[peer],
                    device_id=(tm, z),
                    device_id_type=MESH,
                ).wait()

            return 0

        lax.fori_loop(0, tms, body, 0)

    own.wait()
    for step in [*range(2, chans), 0, 1]:
        finish_group(step)


def local(tms, chans, samples, taps):
    pols, frames, nfft = samples.shape
    tap_count = taps.shape[0]
    count = tms * chans
    per_dev = nfft // 2 // count
    coarse, fine = base_tables(nfft, per_dev, count)
    coarse = coarse.reshape(2, tms, chans, nfft // 2).transpose(2, 0, 1, 3)
    vmem = pl.BlockSpec(memory_space=pltpu.VMEM)
    hbm = pl.BlockSpec(memory_space=pl.ANY)
    return pl.pallas_call(
        functools.partial(kernel, tms, chans),
        out_shape=pltpu.VMEM((2, pols, per_dev, frames * count), jnp.bfloat16),
        in_specs=[hbm, hbm, hbm, hbm],
        out_specs=vmem,
        scratch_shapes=[
            pltpu.VMEM((pols, HALO + frames, nfft), jnp.bfloat16),
            pltpu.VMEM((tap_count, nfft), jnp.float32),
            pltpu.VMEM((chans, 2, tms, nfft // 2), jnp.float32),
            pltpu.VMEM((2, per_dev, nfft // 2), jnp.float32),
            pltpu.VMEM((2, HALO + ROWS, LANES), jnp.float32),
            pltpu.VMEM((frames // 2, nfft), jnp.bfloat16),
            pltpu.VMEM((chans, tms, 2, per_dev, nfft), jnp.bfloat16),
            pltpu.VMEM((chans, tms, 2, pols, per_dev, frames), jnp.bfloat16),
            pltpu.SemaphoreType.DMA((2 * pols + 1,)),
            pltpu.SemaphoreType.DMA((3,)),
            pltpu.SemaphoreType.DMA((chans,)),
            pltpu.SemaphoreType.DMA((2,)),
            pltpu.SemaphoreType.DMA,
            pltpu.SemaphoreType.DMA((count,)),
            pltpu.SemaphoreType.DMA((count,)),
            pltpu.SemaphoreType.REGULAR((2,)),
        ],
        compiler_params=pltpu.CompilerParams(
            collective_id=0, has_side_effects=True, vmem_limit_bytes=56 * 1024 * 1024
        ),
    )(samples, taps, jnp.asarray(coarse), jnp.asarray(fine))


def solution(mesh):
    return jax.shard_map(
        functools.partial(local, mesh.shape["tm"], mesh.shape["chan"]),
        mesh=mesh,
        in_specs=(P(None, ("tm", "chan"), None), P()),
        out_specs=P(None, None, ("tm", "chan"), None),
        check_vma=False,
    )
```
